32 devices in a mesh: tm: 2 (over x), src: 16 (over z, y, core).
Axes of the slice: x: 2, y: 2, z: 4, core: 2. Of those that a mesh axis runs over, the one named last changes fastest.
Arguments:
- design: float32 [16, 524288], P(None, ('tm', 'src')), may hold values from -2 to 2
- unit_index: int32 [524288], P(('tm', 'src')), may hold values from 0 to 255, as said below
- residual: float32 [524288], P(('tm', 'src')), may hold values from -6 to 6
- weight: float32 [524288], P(('tm', 'src')), may hold values from 0.25 to 4
- obs_count: int32 [32], P(('tm', 'src')), may hold values from 1 to 16384, as said below
- damping: float32 [256], P(('tm', 'src')), may hold values from 1 to 10
Outputs:
- solution: float32 [16, 256], P(None, ('tm', 'src'))
- misfit: float32 [], replicated
The draws below stay inside these ranges and needn't reach their ends.
Inputs may be any that keep to these rules, and one draw needn't show every extreme that they name: `unit_index`: an observation on a device of tm index g names a unit in [g * 128, (g + 1) * 128). `obs_count`: some device has all 16384 slots live.
All inputs are finite; a program needn't handle non-finite values.
Results may differ from the reference program's by a relative error of at most 0.0003.
Values sent between devices are 32-bit elements; how exact they have to be, the bound alone decides.
A program may use at most 64 MiB of HBM per device.

```python
import math
import jax
import jax.numpy as jnp
from jax import lax

WIDTH = 16
OBS_DEV = 16384
UNITS_GRP = 128
UNITS = 256
OBS_ALL = 524288
N_SRC = 16
DEVICES = 32


def draw_unit_index(key, part):
    total = OBS_DEV * DEVICES
    group = jnp.arange(total, dtype=jnp.int32) // (OBS_DEV * N_SRC)
    picks = jax.random.randint(jax.random.fold_in(key, 11), (total,), 0, UNITS_GRP, dtype=jnp.int32)
    return picks + group * UNITS_GRP


def draw_obs_count(key, part):
    counts = jax.random.randint(jax.random.fold_in(key, 23), (DEVICES,), OBS_DEV // 8, OBS_DEV // 2 + 1, dtype=jnp.int32)
    return counts.at[0].set(OBS_DEV)


def block_scale(stream_key, extent, shards, least, top_value):
    def one(axis_at, blocks):
        steps = jax.random.uniform(jax.random.fold_in(jax.random.fold_in(stream_key, 6), axis_at), (blocks,), jnp.float32, least / len(shards), top_value / len(shards))
        return jnp.repeat(jnp.exp(steps), extent[axis_at] // blocks).reshape((-1,) + (1,) * (len(extent) - axis_at - 1))

    factor_of = one(*shards[0])
    for cut in shards[1:]:
        factor_of = factor_of * one(*cut)
    return factor_of


def bell_draw(own_key, dims, spread, bound, pieces=(), held_as=jnp.bfloat16):
    entries = spread * jax.random.normal(own_key, dims, jnp.float32)
    if pieces:
        entries = entries * block_scale(own_key, dims, pieces, -0.22, 0.18)
    return jnp.clip(entries, -bound, bound).astype(held_as)


def setup_inputs(seed: int = 0) -> dict:
    key_of = jax.random.split(jax.random.key(seed), 7)
    design = bell_draw(key_of[0], (WIDTH, OBS_ALL), 0.25, 2.0, ((1, 32),), jnp.float32)
    unit_index = draw_unit_index(jax.random.fold_in(key_of[6], 71), 0)
    residual = bell_draw(key_of[2], (OBS_ALL,), 1.0, 6.0, ((0, 32),), jnp.float32)
    weight = jnp.clip(jnp.exp(math.log(4.0) - 2.7725887 * jax.random.uniform(key_of[3], (OBS_ALL,), jnp.float32) ** block_scale(key_of[3], (OBS_ALL,), ((0, 32),), -0.2, 0.2)), 0.25, 4.0)
    obs_count = draw_obs_count(jax.random.fold_in(key_of[6], 71), 0)
    damping = jnp.clip(jnp.exp(math.log(10.0) - 2.3025851 * jax.random.uniform(key_of[5], (UNITS,), jnp.float32) ** block_scale(key_of[5], (UNITS,), ((0, 32),), -0.2, 0.2)), 1.0, 10.0)
    return dict(design=design, unit_index=unit_index, residual=residual, weight=weight, obs_count=obs_count, damping=damping)


def block_solve(normal, rhs, damping):
    lower = {}
    for j in range(16):
        running = normal[j * 16 + j] + damping
        for k in range(j):
            running = running - lower[j, k] * lower[j, k]
        diag_term = jnp.sqrt(running)
        lower[j, j] = diag_term
        for i in range(j + 1, 16):
            running = normal[i * 16 + j]
            for k in range(j):
                running = running - lower[i, k] * lower[j, k]
            lower[i, j] = running / diag_term
    forward = []
    for i in range(16):
        running = rhs[i]
        for k in range(i):
            running = running - lower[i, k] * forward[k]
        forward.append(running / lower[i, i])
    backward = [None] * 16
    for i in range(15, -1, -1):
        running = forward[i]
        for k in range(i + 1, 16):
            running = running - lower[k, i] * backward[k]
        backward[i] = running / lower[i, i]
    return jnp.stack(backward)

def reference(design, unit_index, residual, weight, obs_count, damping):
    units = damping.shape[0]
    blocks = obs_count.shape[0]
    design_blocks = design.reshape(16, blocks, -1).transpose(1, 0, 2)
    unit_blocks = unit_index.reshape(blocks, -1)
    resid_blocks = residual.reshape(blocks, -1)
    weight_blocks = weight.reshape(blocks, -1)
    slots = design_blocks.shape[2]

    def accumulate(carry, item):
        normal_sum, rhs_sum, weight_sum = carry
        rows, units_of, resid, weights, count = item
        weights_on = jnp.where(jnp.arange(slots, dtype=jnp.int32) < count, weights, jnp.zeros_like(weights))
        outer = (rows[:, None, :] * rows[None, :, :]).reshape(256, slots) * weights_on
        normal_sum = normal_sum.at[:, units_of].add(outer)
        rhs_sum = rhs_sum.at[:, units_of].add(rows * (weights_on * resid))
        return ((normal_sum, rhs_sum, weight_sum + jnp.sum(weights_on)), None)
    start = (jnp.zeros((256, units), jnp.float32), jnp.zeros((16, units), jnp.float32), jnp.zeros((), jnp.float32))
    (normal, rhs, weight_total), _ = lax.scan(accumulate, start, (design_blocks, unit_blocks, resid_blocks, weight_blocks, obs_count))
    solution = block_solve(normal, rhs, damping)

    def squares(carry, item):
        rows, units_of, resid, weights, count = item
        weights_on = jnp.where(jnp.arange(slots, dtype=jnp.int32) < count, weights, jnp.zeros_like(weights))
        fitted = lax.optimization_barrier(jnp.sum(rows * solution[:, units_of], axis=0))
        after = resid - fitted
        return (carry + jnp.sum(weights_on * after * after), None)
    chi_total, _ = lax.scan(squares, jnp.zeros((), jnp.float32), (design_blocks, unit_blocks, resid_blocks, weight_blocks, obs_count))
    return (solution, chi_total / weight_total)
```

```python
import functools

import jax
import jax.numpy as jnp
from jax import lax
from jax.experimental import pallas as pl
from jax.experimental.pallas import tpu as pltpu
from jax.sharding import PartitionSpec as P

WIDTH = 16
HALF = 8
PAIRS = WIDTH * (WIDTH + 1) // 2
ROWS = PAIRS + WIDTH
LANES = 128
ROWS_PAD = 256


def pair_row(i, j):
    k = (j - i) % WIDTH
    if k > HALF or (k == HALF and i >= HALF):
        i, j = j, i
        k = (j - i) % WIDTH
    return k * WIDTH + i


def stacked_rows(d0, d1, w, wr):
    w0, w1 = d0 * w, d1 * w
    rows = [d0 * w0, d1 * w1]
    sub = lax.broadcasted_iota(jnp.int32, d0.shape, 0)
    for k in range(1, HALF):
        r0 = pltpu.roll(w0, HALF - k, 0)
        r1 = pltpu.roll(w1, HALF - k, 0)
        low = sub < HALF - k
        rows.append(d0 * jnp.where(low, r0, r1))
        rows.append(d1 * jnp.where(low, r1, r0))
    rows.append(d0 * w1)
    rows.append(d0 * wr)
    rows.append(d1 * wr)
    return rows


def rsqrt(value):
    guess = lax.rsqrt(value)
    return guess * (1.5 - 0.5 * value * guess * guess)


def solve(entry, rhs, damping):
    a = {}
    for i in range(WIDTH):
        for j in range(i + 1):
            a[i, j] = entry(i, j)
        a[i, i] = a[i, i] + damping
    b = [rhs(i) for i in range(WIDTH)]
    inverse, forward = [], []
    for j in range(WIDTH):
        inv = rsqrt(a[j, j])
        inverse.append(inv)
        for i in range(j + 1, WIDTH):
            a[i, j] = a[i, j] * inv
        y = b[j] * inv
        forward.append(y)
        for i in range(j + 1, WIDTH):
            b[i] = b[i] - a[i, j] * y
            for k in range(j + 1, i + 1):
                a[i, k] = a[i, k] - a[i, j] * a[k, j]
    run = list(forward)
    x = [None] * WIDTH
    for i in reversed(range(WIDTH)):
        x[i] = run[i] * inverse[i]
        for k in range(i):
            run[k] = run[k] - a[i, k] * x[i]
    return x, forward


def kernel(
    n_tm, n_src, chunk,
    count_ref, design_ref, unit_ref, resid_ref, weight_ref, damp_ref,
    x_ref, misfit_ref,
    acc, part, got, summed, mine, heard,
    send_a, recv_a, send_b, recv_b,
):
    tm, src = lax.axis_index("tm"), lax.axis_index("src")
    n_all = n_tm * n_src
    me = tm * n_src + src
    own = damp_ref.shape[1]
    units = own * n_src
    slots = design_ref.shape[1]

    def place(flat):
        return {"tm": flat // n_src, "src": flat % n_src}

    barrier = pltpu.get_barrier_semaphore()

    def greet(p, c):
        pl.semaphore_signal(
            barrier, inc=1, device_id=place((me + p) % n_all), device_id_type=pl.DeviceIdType.MESH
        )
        return c

    lax.fori_loop(1, n_all, greet, 0)

    count = count_ref[0]
    first_unit = tm * units
    acc[...] = jnp.zeros_like(acc)

    def accumulate(step, carry):
        chi, total = carry
        begin = pl.multiple_of(step * chunk, chunk)
        cols = pl.ds(begin, chunk)
        w = weight_ref[:, cols]
        live = begin + lax.broadcasted_iota(jnp.int32, w.shape, 1) < count
        w = jnp.where(live, w, 0.0)
        r = resid_ref[:, cols]
        wr = w * r
        rows = stacked_rows(design_ref[0:HALF, cols], design_ref[HALF:WIDTH, cols], w, wr)
        x = jnp.concatenate(rows, axis=0)
        high = x.astype(jnp.bfloat16).astype(jnp.float32)
        lhs = jnp.concatenate([high, x - high], axis=0).astype(jnp.bfloat16)
        unit = unit_ref[:, cols] - first_unit
        hot = lax.broadcasted_iota(jnp.int32, (units, chunk), 0) == unit
        hot = jnp.where(hot, 1.0, 0.0).astype(jnp.bfloat16)
        acc[...] += lax.dot_general(
            lhs, hot, (((1,), (1,)), ((), ())), preferred_element_type=jnp.float32
        )
        wrr = wr * r
        for t in range(chunk // LANES):
            chi = chi + wrr[:, t * LANES:(t + 1) * LANES]
            total = total + w[:, t * LANES:(t + 1) * LANES]
        return chi, total

    zero = jnp.zeros((1, LANES), jnp.float32)
    chi, total = lax.fori_loop(0, slots // chunk, accumulate, (zero, zero))

    sums = acc[0:ROWS] + acc[ROWS:2 * ROWS]
    sums = jnp.concatenate([sums, jnp.zeros((ROWS_PAD - ROWS, units), jnp.float32)], axis=0)
    part[...] = jnp.transpose(sums).reshape(n_src, own, ROWS_PAD)

    pl.semaphore_wait(barrier, n_all - 1)

    def exchange(p):
        to = (src + p) % n_src
        return pltpu.make_async_remote_copy(
            src_ref=part.at[to], dst_ref=got.at[src],
            send_sem=send_a.at[to], recv_sem=recv_a.at[src],
            device_id={"tm": tm, "src": to}, device_id_type=pl.DeviceIdType.MESH,
        )

    def arrival(p):
        frm = (src + p) % n_src
        return frm, pltpu.make_async_remote_copy(
            src_ref=part.at[frm], dst_ref=got.at[frm],
            send_sem=send_a.at[frm], recv_sem=recv_a.at[frm],
            device_id={"tm": tm, "src": frm}, device_id_type=pl.DeviceIdType.MESH,
        )

    def send_one(p, c):
        exchange(p).start()
        return c

    lax.fori_loop(1, n_src, send_one, 0)

    def take_one(p, value):
        frm, copy = arrival(p)
        copy.wait_recv()
        return value + got[frm]

    whole = lax.fori_loop(1, n_src, take_one, part[src])
    summed[...] = jnp.transpose(whole)

    damping = damp_ref[...]
    x, forward = solve(
        lambda i, j: summed[pl.ds(pair_row(i, j), 1), :],
        lambda i: summed[pl.ds(PAIRS + i, 1), :],
        damping,
    )
    terms = jnp.zeros_like(damping)
    squared = jnp.zeros_like(damping)
    for i in range(WIDTH):
        x_ref[i:i + 1, :] = x[i]
        terms = terms + forward[i] * forward[i]
        squared = squared + x[i] * x[i]
    terms = terms + damping * squared
    chi = chi - jnp.concatenate([terms, jnp.zeros((1, LANES - own), jnp.float32)], axis=1)
    lane = lax.broadcasted_iota(jnp.int32, (1, LANES), 1)
    front = lane < LANES // 2
    chi = chi + pltpu.roll(chi, LANES // 2, 1)
    total = total + pltpu.roll(total, LANES // 2, 1)
    mine[...] = jnp.where(front, chi, total)

    def tell(p, c):
        to = (me + p) % n_all
        pltpu.make_async_remote_copy(
            src_ref=mine, dst_ref=heard.at[me],
            send_sem=send_b.at[to], recv_sem=recv_b.at[me],
            device_id=place(to), device_id_type=pl.DeviceIdType.MESH,
        ).start()
        return c

    lax.fori_loop(1, n_all, tell, 0)

    def hear(p, value):
        frm = (me + p) % n_all
        copy = pltpu.make_async_remote_copy(
            src_ref=mine, dst_ref=heard.at[frm],
            send_sem=send_b.at[frm], recv_sem=recv_b.at[frm],
            device_id=place(frm), device_id_type=pl.DeviceIdType.MESH,
        )
        copy.wait_recv()
        return value + heard[frm]

    both = lax.fori_loop(1, n_all, hear, mine[...])
    chi_all = jnp.sum(jnp.where(front, both, 0.0), axis=1, keepdims=True)
    total_all = jnp.sum(jnp.where(front, 0.0, both), axis=1, keepdims=True)
    misfit_ref[...] = chi_all / total_all

    def drain_a(p, c):
        exchange(p).wait_send()
        return c

    lax.fori_loop(1, n_src, drain_a, 0)

    def drain_b(p, c):
        to = (me + p) % n_all
        pltpu.make_async_remote_copy(
            src_ref=mine, dst_ref=heard.at[me],
            send_sem=send_b.at[to], recv_sem=recv_b.at[me],
            device_id=place(to), device_id_type=pl.DeviceIdType.MESH,
        ).wait_send()
        return c

    lax.fori_loop(1, n_all, drain_b, 0)


def solution(mesh):
    n_tm, n_src = mesh.shape["tm"], mesh.shape["src"]
    n_all = n_tm * n_src

    def on_device(design, unit_index, residual, weight, obs_count, damping):
        own = damping.shape[0]
        units = own * n_src
        slots = design.shape[1]
        chunk = 2048 if slots % 2048 == 0 else LANES
        vmem = pl.BlockSpec(memory_space=pltpu.VMEM)
        x, misfit = pl.pallas_call(
            functools.partial(kernel, n_tm, n_src, chunk),
            out_shape=(
                jax.ShapeDtypeStruct((WIDTH, own), jnp.float32),
                jax.ShapeDtypeStruct((1, 1), jnp.float32),
            ),
            in_specs=[pl.BlockSpec(memory_space=pltpu.SMEM)] + [vmem] * 5,
            out_specs=(vmem, vmem),
            scratch_shapes=[
                pltpu.VMEM((2 * ROWS, units), jnp.float32),
                pltpu.VMEM((n_src, own, ROWS_PAD), jnp.float32),
                pltpu.VMEM((n_src, own, ROWS_PAD), jnp.float32),
                pltpu.VMEM((ROWS_PAD, own), jnp.float32),
                pltpu.VMEM((1, LANES), jnp.float32),
                pltpu.VMEM((n_all, 1, LANES), jnp.float32),
                pltpu.SemaphoreType.DMA((n_src,)),
                pltpu.SemaphoreType.DMA((n_src,)),
                pltpu.SemaphoreType.DMA((n_all,)),
                pltpu.SemaphoreType.DMA((n_all,)),
            ],
            compiler_params=pltpu.CompilerParams(collective_id=0, has_side_effects=True),
            name="calibrate",
        )(
            obs_count,
            design,
            unit_index.reshape(1, slots),
            residual.reshape(1, slots),
            weight.reshape(1, slots),
            damping.reshape(1, own),
        )
        return x, misfit.reshape(())

    both = ("tm", "src")
    return jax.shard_map(
        on_device,
        mesh=mesh,
        in_specs=(P(None, both), P(both), P(both), P(both), P(both), P(both)),
        out_specs=(P(None, both), P()),
        check_vma=False,
    )
```

```python
import functools

import jax
import jax.numpy as jnp
from jax import lax
from jax.experimental import pallas as pl
from jax.experimental.pallas import tpu as pltpu
from jax.sharding import PartitionSpec as P

WIDTH = 16
HALF = 8
PAIRS = WIDTH * (WIDTH + 1) // 2
ROWS = PAIRS + WIDTH
LANES = 128
FOLD = 4


def pair_row(i, j):
    k = (j - i) % WIDTH
    if k > HALF or (k == HALF and i >= HALF):
        i, j = j, i
        k = (j - i) % WIDTH
    return k * WIDTH + i


def stacked_rows(d0, d1, w, wr):
    w0, w1 = d0 * w, d1 * w
    rows = [d0 * w0, d1 * w1]
    sub = lax.broadcasted_iota(jnp.int32, d0.shape, 0)
    for k in range(1, HALF):
        r0 = pltpu.roll(w0, HALF - k, 0)
        r1 = pltpu.roll(w1, HALF - k, 0)
        low = sub < HALF - k
        rows.append(d0 * jnp.where(low, r0, r1))
        rows.append(d1 * jnp.where(low, r1, r0))
    rows.append(d0 * w1)
    rows.append(d0 * wr)
    rows.append(d1 * wr)
    return rows


def rsqrt(value):
    guess = lax.rsqrt(value)
    return guess * (1.5 - 0.5 * value * guess * guess)


def solve(entry, rhs, damping):
    a = {}
    for i in range(WIDTH):
        for j in range(i + 1):
            a[i, j] = entry(i, j)
        a[i, i] = a[i, i] + damping
    b = [rhs(i) for i in range(WIDTH)]
    inverse, forward = [], []
    for j in range(WIDTH):
        inv = rsqrt(a[j, j])
        inverse.append(inv)
        for i in range(j + 1, WIDTH):
            a[i, j] = a[i, j] * inv
        y = b[j] * inv
        forward.append(y)
        for i in range(j + 1, WIDTH):
            b[i] = b[i] - a[i, j] * y
            for k in range(j + 1, i + 1):
                a[i, k] = a[i, k] - a[i, j] * a[k, j]
    run = list(forward)
    x = [None] * WIDTH
    for i in reversed(range(WIDTH)):
        x[i] = run[i] * inverse[i]
        for k in range(i):
            run[k] = run[k] - a[i, k] * x[i]
    return x, forward


def far_first(n):
    q = max(n // 4, 1)
    order = []
    for i in range(q):
        order += [3 * q + i, q + i]
    order += list(range(2 * q, 3 * q)) + list(range(1, q))
    return [p for p in dict.fromkeys(order) if 0 < p < n]


def each(pairs, body, start):
    if len(pairs) <= 32:
        for dt, dp in pairs:
            start = body(dt, dp, start)
        return start
    n_src = max(dp for _, dp in pairs) + 1
    return lax.fori_loop(
        1, len(pairs) + 1, lambda i, c: body(i // n_src, i % n_src, c), start
    )


def kernel(
    n_tm, n_src, chunk,
    count_hbm, design_hbm, unit_hbm, resid_hbm, weight_hbm, damp_hbm,
    x_ref, misfit_ref,
    count_ref, design_ref, unit_ref, resid_ref, weight_ref, damp_ref,
    acc, extra, part, tail, got, got_tail, summed, spread, mine, heard,
    load, small, send_a, recv_a, send_b, recv_b,
):
    tm, src = lax.axis_index("tm"), lax.axis_index("src")
    n_all = n_tm * n_src
    me = tm * n_src + src
    own = damp_ref.shape[1]
    units = own * n_src
    slots = design_ref.shape[1]
    turns = slots // chunk
    order = far_first(n_src)
    near = [(0, p) for p in order]
    everyone = [(dt, p) for dt in range(n_tm - 1, 0, -1) for p in order + [0]] + near

    arrays = (
        (design_hbm, design_ref), (unit_hbm, unit_ref),
        (resid_hbm, resid_ref), (weight_hbm, weight_ref),
    )

    def fetch(step, which):
        far, here = arrays[which]
        cols = pl.ds(pl.multiple_of(step * chunk, chunk), chunk)
        return pltpu.make_async_copy(far.at[:, cols], here.at[:, cols], load.at[step, which])

    count_copy = pltpu.make_async_copy(count_hbm, count_ref, small.at[0])
    damp_copy = pltpu.make_async_copy(damp_hbm, damp_ref, small.at[1])
    count_copy.start()
    for which in range(4):
        fetch(0, which).start()
    for step in range(1, turns):
        for which in range(4):
            fetch(step, which).start()
    damp_copy.start()

    def at(dt, dp):
        return {"tm": (tm + dt) % n_tm, "src": (src + dp) % n_src}

    barrier = pltpu.get_barrier_semaphore()

    def greet(dt, dp, c):
        pl.semaphore_signal(
            barrier, inc=1, device_id=at(dt, dp), device_id_type=pl.DeviceIdType.MESH
        )
        return c

    each(everyone, greet, 0)

    first_unit = tm * units
    zero = jnp.zeros((1, LANES), jnp.float32)
    count_copy.wait()
    count = count_ref[0]

    def accumulate(step, carry):
        chi, total = carry
        for which in range(4):
            fetch(step, which).wait()
        begin = pl.multiple_of(step * chunk, chunk)
        cols = pl.ds(begin, chunk)
        w = weight_ref[:, cols]
        live = begin + lax.broadcasted_iota(jnp.int32, w.shape, 1) < count
        w = jnp.where(live, w, 0.0)
        r = resid_ref[:, cols]
        wr = w * r
        rows = stacked_rows(design_ref[0:HALF, cols], design_ref[HALF:WIDTH, cols], w, wr)
        x = jnp.concatenate(rows, axis=0)
        high = x.astype(jnp.bfloat16).astype(jnp.float32)
        lhs = jnp.concatenate([high, x - high], axis=0).astype(jnp.bfloat16)
        unit = unit_ref[:, cols] - first_unit
        hot = lax.broadcasted_iota(jnp.int32, (units, chunk), 0) == unit
        hot = jnp.where(hot, 1.0, 0.0).astype(jnp.bfloat16)
        acc[...] += lax.dot_general(
            lhs, hot, (((1,), (1,)), ((), ())), preferred_element_type=jnp.float32
        )
        wrr = wr * r
        for t in range(chunk // LANES):
            chi = chi + wrr[:, t * LANES:(t + 1) * LANES]
            total = total + w[:, t * LANES:(t + 1) * LANES]
        return chi, total

    acc[...] = jnp.zeros_like(acc)
    chi, total = lax.fori_loop(0, turns, accumulate, (zero, zero))

    sums = acc[0:ROWS] + acc[ROWS:2 * ROWS]
    left = jnp.concatenate(
        [sums[LANES:ROWS], jnp.zeros((2 * LANES - ROWS, units), jnp.float32)], axis=0
    )
    extra[...] = jnp.transpose(left)
    part[...] = jnp.transpose(sums[0:LANES]).reshape(n_src, own, LANES)
    packed = extra[pl.ds(0, units // FOLD, stride=FOLD), :]
    for b in range(1, FOLD):
        packed = packed + pltpu.roll(
            extra[pl.ds(b, units // FOLD, stride=FOLD), :], b * (LANES // FOLD), 1
        )
    tail[...] = packed.reshape(n_src, own // FOLD, LANES)

    pl.semaphore_wait(barrier, n_all - 1)

    def exchange(peer, slot, which):
        mine_of, theirs = ((part, got), (tail, got_tail))[which]
        return pltpu.make_async_remote_copy(
            src_ref=mine_of.at[peer], dst_ref=theirs.at[slot],
            send_sem=send_a.at[which, peer], recv_sem=recv_a.at[which, slot],
            device_id={"tm": tm, "src": peer}, device_id_type=pl.DeviceIdType.MESH,
        )

    def send_one(dt, dp, c):
        to = (src + dp) % n_src
        exchange(to, src, 0).start()
        exchange(to, src, 1).start()
        return c

    each(near, send_one, 0)

    def take_one(dt, dp, carry):
        frm = (src - dp + n_src) % n_src
        exchange(frm, frm, 0).wait_recv()
        exchange(frm, frm, 1).wait_recv()
        return carry[0] + got[frm], carry[1] + got_tail[frm]

    whole, ends = each(list(reversed(near)), take_one, (part[src], tail[src]))
    for a in range(own // FOLD):
        for b in range(FOLD):
            row = ends[a:a + 1]
            spread[pl.ds(a * FOLD + b, 1), :] = (
                pltpu.roll(row, LANES - b * (LANES // FOLD), 1) if b else row
            )
    summed[0:LANES, :] = jnp.transpose(whole)
    summed[LANES:2 * LANES, :] = jnp.transpose(spread[...])

    damp_copy.wait()
    damping = damp_ref[...]
    x, forward = solve(
        lambda i, j: summed[pl.ds(pair_row(i, j), 1), :],
        lambda i: summed[pl.ds(PAIRS + i, 1), :],
        damping,
    )
    terms = jnp.zeros_like(damping)
    squared = jnp.zeros_like(damping)
    for i in range(WIDTH):
        terms = terms + forward[i] * forward[i]
        squared = squared + x[i] * x[i]
    terms = terms + damping * squared
    chi = chi - jnp.concatenate([terms, jnp.zeros((1, LANES - own), jnp.float32)], axis=1)
    lane = lax.broadcasted_iota(jnp.int32, (1, LANES), 1)
    front = lane < LANES // 2
    chi = chi + pltpu.roll(chi, LANES // 2, 1)
    total = total + pltpu.roll(total, LANES // 2, 1)
    mine[...] = jnp.where(front, chi, total)

    def tell(dt, dp):
        to = ((tm + dt) % n_tm) * n_src + (src + dp) % n_src
        return pltpu.make_async_remote_copy(
            src_ref=mine, dst_ref=heard.at[me],
            send_sem=send_b.at[to], recv_sem=recv_b.at[me],
            device_id=at(dt, dp), device_id_type=pl.DeviceIdType.MESH,
        )

    def tell_one(dt, dp, c):
        tell(dt, dp).start()
        return c

    each(everyone, tell_one, 0)

    x_ref[...] = jnp.transpose(jnp.concatenate(x, axis=0))

    def hear_one(dt, dp, value):
        frm = ((tm + dt) % n_tm) * n_src + (src + dp) % n_src
        pltpu.make_async_remote_copy(
            src_ref=mine, dst_ref=heard.at[frm],
            send_sem=send_b.at[frm], recv_sem=recv_b.at[frm],
            device_id=at(dt, dp), device_id_type=pl.DeviceIdType.MESH,
        ).wait_recv()
        return value + heard[frm]

    def drain_a(dt, dp, c):
        to = (src + dp) % n_src
        exchange(to, src, 0).wait_send()
        exchange(to, src, 1).wait_send()
        return c

    each(near, drain_a, 0)
    both = each(list(reversed(everyone)), hear_one, mine[...])
    chi_all = jnp.sum(jnp.where(front, both, 0.0), axis=1, keepdims=True)
    total_all = jnp.sum(jnp.where(front, 0.0, both), axis=1, keepdims=True)
    misfit_ref[...] = chi_all / total_all

    def drain_b(dt, dp, c):
        tell(dt, dp).wait_send()
        return c

    each(everyone, drain_b, 0)


def hand_on(x_ref, misfit_ref, x_out, misfit_out):
    x_out[...] = x_ref[...]
    misfit_out[...] = misfit_ref[...]


def solution(mesh):
    n_tm, n_src = mesh.shape["tm"], mesh.shape["src"]
    n_all = n_tm * n_src

    def on_device(design, unit_index, residual, weight, obs_count, damping):
        own = damping.shape[0]
        units = own * n_src
        slots = design.shape[1]
        chunk = 8192 if slots % 8192 == 0 else LANES
        turns = slots // chunk
        anywhere = pl.BlockSpec(memory_space=pl.ANY)
        vmem = pl.BlockSpec(memory_space=pltpu.VMEM)
        x, misfit = pl.pallas_call(
            functools.partial(kernel, n_tm, n_src, chunk),
            out_shape=(
                jax.ShapeDtypeStruct((own, WIDTH), jnp.float32),
                jax.ShapeDtypeStruct((1, 1), jnp.float32),
            ),
            in_specs=[anywhere] * 6,
            out_specs=(vmem, vmem),
            scratch_shapes=[
                pltpu.SMEM((1,), jnp.int32),
                pltpu.VMEM((WIDTH, slots), jnp.float32),
                pltpu.VMEM((1, slots), jnp.int32),
                pltpu.VMEM((1, slots), jnp.float32),
                pltpu.VMEM((1, slots), jnp.float32),
                pltpu.VMEM((1, own), jnp.float32),
                pltpu.VMEM((2 * ROWS, units), jnp.float32),
                pltpu.VMEM((units, LANES), jnp.float32),
                pltpu.VMEM((n_src, own, LANES), jnp.float32),
                pltpu.VMEM((n_src, own // FOLD, LANES), jnp.float32),
                pltpu.VMEM((n_src, own, LANES), jnp.float32),
                pltpu.VMEM((n_src, own // FOLD, LANES), jnp.float32),
                pltpu.VMEM((2 * LANES, own), jnp.float32),
                pltpu.VMEM((own, LANES), jnp.float32),
                pltpu.VMEM((1, LANES), jnp.float32),
                pltpu.VMEM((n_all, 1, LANES), jnp.float32),
                pltpu.SemaphoreType.DMA((turns, 4)),
                pltpu.SemaphoreType.DMA((2,)),
                pltpu.SemaphoreType.DMA((2, n_src)),
                pltpu.SemaphoreType.DMA((2, n_src)),
                pltpu.SemaphoreType.DMA((n_all,)),
                pltpu.SemaphoreType.DMA((n_all,)),
            ],
            compiler_params=pltpu.CompilerParams(collective_id=0, has_side_effects=True),
            name="calibrate",
        )(
            obs_count,
            design,
            unit_index.reshape(1, slots),
            residual.reshape(1, slots),
            weight.reshape(1, slots),
            damping.reshape(1, own),
        )
        x, misfit = pl.pallas_call(
            hand_on,
            out_shape=(
                jax.ShapeDtypeStruct((own, WIDTH), jnp.float32),
                jax.ShapeDtypeStruct((1, 1), jnp.float32),
            ),
            in_specs=[vmem, vmem],
            out_specs=(vmem, vmem),
            name="hand_on",
        )(x, misfit)
        return x.T, misfit.reshape(())

    both = ("tm", "src")
    return jax.shard_map(
        on_device,
        mesh=mesh,
        in_specs=(P(None, both), P(both), P(both), P(both), P(both), P(both)),
        out_specs=(P(None, both), P()),
        check_vma=False,
    )
```
